256 devices in a mesh: gx: 16 (over x, y_lo, core), gy: 16 (over y_hi, z).
Axes of the slice: x: 4, y: 4 (y_hi: 2, y_lo: 2; y = y_hi * 2 + y_lo), z: 8, core: 2. Of those that a mesh axis runs over, the one named last changes fastest.
Arguments:
- cells: bfloat16 [2048, 1024, 128], P('gx', 'gy'), may hold values from -6 to 6
- cotangent: bfloat16 [2048, 1024, 128], P('gx', 'gy'), may hold values from -6 to 6
- lift_weight: bfloat16 [128, 512], replicated, may hold values from -0.5 to 0.5
- drop_weight: bfloat16 [512, 128], replicated, may hold values from -0.25 to 0.25
- xmode_weight: bfloat16 [2, 16, 128, 128], P(None, 'gx'), may hold values from -0.375 to 0.375
- ymode_weight: bfloat16 [2, 8, 128, 128], replicated, may hold values from -0.375 to 0.375
- coarse_weight: bfloat16 [128, 128], replicated, may hold values from -0.5 to 0.5
- coarse_mix: bfloat16 [64, 64], replicated, may hold values from -0.75 to 0.75
Outputs:
- cell_grad: bfloat16 [2048, 1024, 128], P('gx', 'gy')
- lift_grad: float32 [128, 512], replicated
- drop_grad: float32 [512, 128], replicated
- xmode_grad: float32 [2, 16, 128, 128], P(None, 'gx')
- ymode_grad: float32 [2, 8, 128, 128], replicated
- coarse_weight_grad: float32 [128, 128], replicated
- coarse_mix_grad: float32 [64, 64], replicated
The draws below stay inside these ranges and needn't reach their ends.
All inputs are finite; a program needn't handle non-finite values.
Results may differ from the reference program's by a relative error of at most 0.006.
Values sent between devices are 32-bit elements; how exact they have to be, the bound alone decides.
No kernel may reach another device: no remote copies, remote signals or barrier semaphores. Data moves between devices by JAX's collectives and lax.ppermute only.
A program may use at most 128 MiB of HBM per device.

```python
import math
import jax
import jax.numpy as jnp
from jax import lax

WIDTH = 128
FFN_WIDTH = 512
MODES_X = 16
MODES_Y = 8
POOL = 16
NX = 2048
NY = 1024
NYC = 64


def level_of(own_key, dims, shards, least, high):
    def one(position, shards_of):
        draws = jax.random.uniform(jax.random.fold_in(jax.random.fold_in(own_key, 6), position), (shards_of,), jnp.float32, least / len(shards), high / len(shards))
        return jnp.repeat(jnp.exp(draws), dims[position] // shards_of).reshape((-1,) + (1,) * (len(dims) - position - 1))

    gain = one(*shards[0])
    for cut in shards[1:]:
        gain = gain * one(*cut)
    return gain


def gaussian(rng, shape, deviation, bound, pieces=(), kind=jnp.bfloat16):
    result = deviation * jax.random.normal(rng, shape, jnp.float32)
    if pieces:
        result = result * level_of(rng, shape, pieces, -0.22, 0.18)
    return jnp.clip(result, -bound, bound).astype(kind)


def setup_inputs(seed: int = 0) -> dict:
    seeds = jax.random.split(jax.random.key(seed), 9)
    cells = gaussian(seeds[0], (NX, NY, WIDTH), 1.0, 6.0, ((0, 16), (1, 16)))
    cotangent = gaussian(seeds[1], (NX, NY, WIDTH), 1.0, 6.0, ((0, 16), (1, 16)))
    lift_weight = gaussian(seeds[2], (WIDTH, FFN_WIDTH), WIDTH ** -0.5, 0.5)
    drop_weight = gaussian(seeds[3], (FFN_WIDTH, WIDTH), FFN_WIDTH ** -0.5, 0.25)
    xmode_weight = gaussian(seeds[4], (2, MODES_X, WIDTH, WIDTH), (2 * WIDTH) ** -0.5, 0.375, ((1, 16),))
    ymode_weight = gaussian(seeds[5], (2, MODES_Y, WIDTH, WIDTH), (2 * WIDTH) ** -0.5, 0.375)
    coarse_weight = gaussian(seeds[6], (WIDTH, WIDTH), WIDTH ** -0.5, 0.5)
    coarse_mix = gaussian(seeds[7], (NYC, NYC), NYC ** -0.5, 0.75)
    return dict(cells=cells, cotangent=cotangent, lift_weight=lift_weight, drop_weight=drop_weight, xmode_weight=xmode_weight, ymode_weight=ymode_weight, coarse_weight=coarse_weight, coarse_mix=coarse_mix)


gelu_scale = 0.7978845608028654
gelu_cubic = 0.044715
highest = lax.Precision.HIGHEST

def gelu_value(values):
    tangent = jnp.tanh(gelu_scale * (values + gelu_cubic * values * values * values))
    return 0.5 * values * (1.0 + tangent)

def gelu_slope(values):
    tangent = jnp.tanh(gelu_scale * (values + gelu_cubic * values * values * values))
    return 0.5 * (1.0 + tangent) + 0.5 * values * (1.0 - tangent * tangent) * gelu_scale * (1.0 + 3.0 * gelu_cubic * values * values)

def mode_basis(mode_count, length, offset, extent):
    frequency = jnp.arange(mode_count, dtype=jnp.int32)
    places = offset + jnp.arange(extent, dtype=jnp.int32)
    phase_index = frequency[:, None] * places[None, :] % length
    angles = phase_index.astype(jnp.float32) * (2.0 * math.pi / length)
    return jnp.concatenate([jnp.cos(angles), -jnp.sin(angles)], axis=0)

def mix_modes(spectrum, weights):

    def product(former, latter):
        return jnp.einsum('mrc,mcd->mrd', former, latter, precision=highest)
    real_out = product(spectrum[0], weights[0]) - product(spectrum[1], weights[1])
    imaginary_out = product(spectrum[0], weights[1]) + product(spectrum[1], weights[0])
    return jnp.stack([real_out, imaginary_out])

def mix_back(spectrum, gradient, weights):

    def contract_cells(former, latter):
        return jnp.einsum('mrc,mrd->mcd', former, latter, precision=highest)

    def contract_channels(former, latter):
        return jnp.einsum('mrd,mcd->mrc', former, latter, precision=highest)
    weight_real = contract_cells(spectrum[0], gradient[0]) + contract_cells(spectrum[1], gradient[1])
    weight_imaginary = contract_cells(spectrum[0], gradient[1]) - contract_cells(spectrum[1], gradient[0])
    spec_real = contract_channels(gradient[0], weights[0]) + contract_channels(gradient[1], weights[1])
    spec_imaginary = contract_channels(gradient[1], weights[0]) - contract_channels(gradient[0], weights[1])
    return (jnp.stack([weight_real, weight_imaginary]), jnp.stack([spec_real, spec_imaginary]))

def reference(cells, cotangent, lift_weight, drop_weight, xmode_weight, ymode_weight, coarse_weight, coarse_mix):
    block_count = NX // POOL
    row_basis = mode_basis(MODES_X, NX, 0, NX)
    column_basis = mode_basis(MODES_Y, NY, 0, NY)
    column_basis_low = column_basis.astype(jnp.bfloat16).astype(jnp.float32)
    row_weight = xmode_weight.astype(jnp.float32)
    column_weight = ymode_weight.astype(jnp.float32)
    coarse_float = coarse_weight.astype(jnp.float32)
    mixing_float = coarse_mix.astype(jnp.float32)
    row_spec = jnp.dot(row_basis.astype(jnp.bfloat16), cells.reshape(NX, NY * WIDTH), preferred_element_type=jnp.float32) * (1.0 / math.sqrt(NX))
    row_spec = row_spec.reshape(2, MODES_X, NY, WIDTH)
    row_mixed = mix_modes(row_spec, row_weight).reshape(2 * MODES_X, NY * WIDTH)
    cell_blocks = cells.reshape(block_count, POOL, NY, WIDTH)
    cotangent_blocks = cotangent.reshape(block_count, POOL, NY, WIDTH)
    block_ids = jnp.arange(block_count, dtype=jnp.int32)

    def first_pass(cell_block):
        widened = cell_block.astype(jnp.float32)
        spectrum = jnp.einsum('ry,xyc->rxc', column_basis_low, widened, precision=highest)
        pooled_row = widened.reshape(POOL, NYC, POOL, WIDTH).sum(axis=(0, 2)) / POOL
        return (spectrum, pooled_row)
    column_blocks, pooled = lax.map(first_pass, cell_blocks)
    column_spec = column_blocks.transpose(1, 0, 2, 3).reshape(2, MODES_Y, NX, WIDTH) * (1.0 / math.sqrt(NY))
    column_mixed = mix_modes(column_spec, column_weight).reshape(2 * MODES_Y, NX, WIDTH)
    coarse_pre = jnp.einsum('ijc,cd->ijd', pooled, coarse_float, precision=highest)
    coarse_act = gelu_value(coarse_pre)
    coarse_out = jnp.einsum('jk,ikc->ijc', mixing_float, coarse_act, precision=highest)

    def second_pass(totals, inputs):
        lift_total, drop_total, row_total = totals
        block_index, cotangent_block = inputs
        row_offset = block_index * POOL
        basis_rows = lax.dynamic_slice_in_dim(row_basis, row_offset, POOL, 1)
        row_field = jnp.dot(basis_rows.T, row_mixed, precision=highest) * (1.0 / math.sqrt(MODES_X))
        column_rows = lax.dynamic_slice_in_dim(column_mixed, row_offset, POOL, 1)
        column_field = jnp.einsum('ry,rxc->xyc', column_basis, column_rows, precision=highest) * (1.0 / math.sqrt(MODES_Y))
        coarse_row = lax.dynamic_slice_in_dim(coarse_out, block_index, 1, 0)
        lifted = jnp.broadcast_to(coarse_row[:, :, None, :], (1, NYC, POOL, WIDTH)).reshape(1, NY, WIDTH)
        summed = row_field.reshape(POOL, NY, WIDTH) + column_field + lifted
        ffn_input = summed.reshape(POOL * NY, WIDTH).astype(jnp.bfloat16)
        hidden_before = jnp.dot(ffn_input, lift_weight, preferred_element_type=jnp.float32)
        hidden_after = gelu_value(hidden_before).astype(jnp.bfloat16)
        cotangent_rows = cotangent_block.reshape(POOL * NY, WIDTH)
        drop_total = drop_total + jnp.dot(hidden_after.T, cotangent_rows, preferred_element_type=jnp.float32)
        after_grad = jnp.dot(cotangent_rows, drop_weight.T, preferred_element_type=jnp.float32)
        before_grad = (after_grad * gelu_slope(hidden_before)).astype(jnp.bfloat16)
        lift_total = lift_total + jnp.dot(ffn_input.T, before_grad, preferred_element_type=jnp.float32)
        summed_grad = jnp.dot(before_grad, lift_weight.T, preferred_element_type=jnp.float32).reshape(POOL, NY, WIDTH)
        row_total = row_total + jnp.dot(basis_rows, summed_grad.reshape(POOL, NY * WIDTH), precision=highest)
        column_piece = jnp.einsum('ry,xyc->rxc', column_basis, summed_grad, precision=highest)
        coarse_piece = summed_grad.reshape(POOL, NYC, POOL, WIDTH).sum(axis=(0, 2))
        return ((lift_total, drop_total, row_total), (column_piece, coarse_piece))
    initial = (jnp.zeros((WIDTH, FFN_WIDTH), jnp.float32), jnp.zeros((FFN_WIDTH, WIDTH), jnp.float32), jnp.zeros((2 * MODES_X, NY * WIDTH), jnp.float32))
    (lift_grad, drop_grad, row_sum), (column_pieces, coarse_grad) = lax.scan(second_pass, initial, (block_ids, cotangent_blocks))
    row_back = row_sum.reshape(2, MODES_X, NY, WIDTH) * (1.0 / math.sqrt(MODES_X))
    column_back = column_pieces.transpose(1, 0, 2, 3).reshape(2, MODES_Y, NX, WIDTH) * (1.0 / math.sqrt(MODES_Y))
    xmode_grad, row_spec_grad = mix_back(row_spec, row_back, row_weight)
    ymode_grad, column_spec_grad = mix_back(column_spec, column_back, column_weight)
    coarse_act_grad = jnp.einsum('jk,ijc->ikc', mixing_float, coarse_grad, precision=highest)
    coarse_mix_grad = jnp.einsum('ijc,ikc->jk', coarse_grad, coarse_act, precision=highest)
    coarse_pre_grad = coarse_act_grad * gelu_slope(coarse_pre)
    coarse_weight_grad = jnp.einsum('ijc,ijd->cd', pooled, coarse_pre_grad, precision=highest)
    pooled_grad = jnp.einsum('ijd,cd->ijc', coarse_pre_grad, coarse_float, precision=highest) * (1.0 / POOL)
    row_flat = row_spec_grad.reshape(2 * MODES_X, NY * WIDTH)
    column_flat = column_spec_grad.reshape(2 * MODES_Y, NX, WIDTH)

    def third_pass(inputs):
        block_index, cotangent_block = inputs
        row_offset = block_index * POOL
        basis_rows = lax.dynamic_slice_in_dim(row_basis, row_offset, POOL, 1)
        row_piece = jnp.dot(basis_rows.T, row_flat, precision=highest).reshape(POOL, NY, WIDTH) * (1.0 / math.sqrt(NX))
        column_rows = lax.dynamic_slice_in_dim(column_flat, row_offset, POOL, 1)
        column_piece = jnp.einsum('ry,rxc->xyc', column_basis, column_rows, precision=highest) * (1.0 / math.sqrt(NY))
        pooled_row = lax.dynamic_slice_in_dim(pooled_grad, block_index, 1, 0)
        lifted = jnp.broadcast_to(pooled_row[:, :, None, :], (1, NYC, POOL, WIDTH)).reshape(1, NY, WIDTH)
        return (cotangent_block.astype(jnp.float32) + row_piece + column_piece + lifted).astype(jnp.bfloat16)
    cell_grad = lax.map(third_pass, (block_ids, cotangent_blocks)).reshape(NX, NY, WIDTH)
    return (cell_grad, lift_grad, drop_grad, xmode_grad, ymode_grad, coarse_weight_grad, coarse_mix_grad)
```

```python
import math

import jax
import jax.numpy as jnp
from jax import lax
from jax.sharding import Mesh
from jax.sharding import PartitionSpec as P

MODES_X = 16
MODES_Y = 8
POOL = 16
GX = ("x", "yl", "co")
GY = ("yh", "z")

gelu_scale = 0.7978845608028654
gelu_cubic = 0.044715
highest = lax.Precision.HIGHEST


def gelu_value(values):
    tangent = jnp.tanh(gelu_scale * (values + gelu_cubic * values * values * values))
    return 0.5 * values * (1.0 + tangent)


def gelu_slope(values):
    tangent = jnp.tanh(gelu_scale * (values + gelu_cubic * values * values * values))
    return 0.5 * (1.0 + tangent) + 0.5 * values * (1.0 - tangent * tangent) * gelu_scale * (
        1.0 + 3.0 * gelu_cubic * values * values
    )


def basis_of(frequency, length, offset, extent):
    places = offset + jnp.arange(extent, dtype=jnp.int32)
    phase_index = frequency[:, None] * places[None, :] % length
    angles = phase_index.astype(jnp.float32) * (2.0 * math.pi / length)
    return jnp.stack([jnp.cos(angles), -jnp.sin(angles)], axis=1)


def x_step(step):
    return [(i, (i + step) % 4) for i in range(4)]


SWAP = [(0, 1), (1, 0)]


def relative_modes():
    j = jnp.arange(16, dtype=jnp.int32)
    x = (lax.axis_index("x") + j % 4) % 4
    yl = (lax.axis_index("yl") + j // 4) % 2
    co = (lax.axis_index("co") + j // 8) % 2
    return x * 4 + yl * 2 + co


def scatter_gx(parts):
    s = parts[:8] + lax.ppermute(parts[8:], "co", SWAP)
    s = s[:4] + lax.ppermute(s[4:], "yl", SWAP)
    arrived = [lax.ppermute(s[k], "x", x_step(k)) for k in (1, 2, 3)]
    return s[0] + arrived[0] + arrived[1] + arrived[2]


def gather_gx(own):
    g = jnp.stack([own] + [lax.ppermute(own, "x", x_step(-k)) for k in (1, 2, 3)])
    g = jnp.concatenate([g, lax.ppermute(g, "yl", SWAP)])
    return jnp.concatenate([g, lax.ppermute(g, "co", SWAP)])


def exchange_gy(parts):
    return lax.all_to_all(parts, GY, 0, 0, tiled=True)


def copies(block, count):
    return jnp.broadcast_to(block[None], (count, *block.shape))


def complex_mix(spectrum, weights):
    def product(former, latter):
        return jnp.einsum("rc,cd->rd", former, latter, precision=highest)

    return jnp.stack(
        [
            product(spectrum[0], weights[0]) - product(spectrum[1], weights[1]),
            product(spectrum[0], weights[1]) + product(spectrum[1], weights[0]),
        ]
    )


def complex_back(spectrum, gradient, weights):
    def over_cells(former, latter):
        return jnp.einsum("rc,rd->cd", former, latter, precision=highest)

    def over_channels(former, latter):
        return jnp.einsum("rd,cd->rc", former, latter, precision=highest)

    weight = jnp.stack(
        [
            over_cells(spectrum[0], gradient[0]) + over_cells(spectrum[1], gradient[1]),
            over_cells(spectrum[0], gradient[1]) - over_cells(spectrum[1], gradient[0]),
        ]
    )
    spec = jnp.stack(
        [
            over_channels(gradient[0], weights[0]) + over_channels(gradient[1], weights[1]),
            over_channels(gradient[1], weights[0]) - over_channels(gradient[0], weights[1]),
        ]
    )
    return weight, spec


def upsample(coarse_field, row_count, column_count, channels):
    spread = jnp.broadcast_to(
        coarse_field[:, None, :, None, :],
        (row_count // POOL, POOL, column_count // POOL, POOL, channels),
    )
    return spread.reshape(row_count, column_count, channels)


def on_device(
    cells,
    cotangent,
    lift_weight,
    drop_weight,
    xmode_weight,
    ymode_weight,
    coarse_weight,
    coarse_mix,
):
    rows, columns, channels = cells.shape
    row_total = rows * 16
    column_total = columns * 16
    coarse_rows = rows // POOL
    coarse_columns = columns // POOL
    half = rows // 2
    cells_flat = rows * columns
    gx = lax.axis_index(GX)
    gy = lax.axis_index(GY)
    order = relative_modes()
    row_basis = basis_of(order, row_total, gx * rows, rows).reshape(32, rows)
    column_basis = basis_of(
        jnp.arange(MODES_Y, dtype=jnp.int32), column_total, gy * columns, columns
    ).reshape(16, columns)
    row_weight = xmode_weight[:, 0].astype(jnp.float32)
    column_weight = lax.dynamic_index_in_dim(ymode_weight, gy // 2, 1, keepdims=False).astype(
        jnp.float32
    )
    coarse_float = coarse_weight.astype(jnp.float32)
    mixing = coarse_mix.astype(jnp.float32)
    own_mixing = lax.dynamic_slice_in_dim(mixing, gy * coarse_columns, coarse_columns, 1)
    units = lift_weight.shape[1] // 16
    lift_turned = jnp.take(lift_weight.T.reshape(16, units, channels), order, axis=0).reshape(
        16 * units, channels
    )
    drop_turned = jnp.take(drop_weight.reshape(16, units, channels), order, axis=0).reshape(
        16 * units, channels
    )

    def to_gy(by_part):
        return (
            by_part.reshape(MODES_Y, 2, 2, half, channels)
            .transpose(0, 2, 1, 3, 4)
            .reshape(16, 2 * half, channels)
        )

    def from_gy(blocks):
        return (
            blocks.reshape(MODES_Y, 2, 2, half, channels)
            .transpose(0, 2, 1, 3, 4)
            .reshape(16, rows, channels)
        )

    row_partial = jnp.dot(
        row_basis.astype(jnp.bfloat16),
        cells.reshape(rows, columns * channels),
        preferred_element_type=jnp.float32,
    ) * (1.0 / math.sqrt(row_total))
    column_partial = jnp.einsum(
        "ry,xyc->rxc", column_basis.astype(jnp.bfloat16), cells, preferred_element_type=jnp.float32
    ) * (1.0 / math.sqrt(column_total))
    pooled = cells.astype(jnp.float32).reshape(
        coarse_rows, POOL, coarse_columns, POOL, channels
    ).sum(axis=(1, 3)) * (1.0 / POOL)
    coarse_pre = jnp.einsum("ijc,cd->ijd", pooled, coarse_float, precision=highest)
    coarse_act = gelu_value(coarse_pre)
    coarse_share = jnp.einsum("jk,ikc->jic", own_mixing, coarse_act, precision=highest)
    coarse_share = coarse_share.reshape(16, coarse_columns * coarse_rows, channels)
    arrived = exchange_gy(
        jnp.concatenate(
            [to_gy(column_partial.reshape(MODES_Y, 2, rows, channels)), coarse_share], axis=1
        )
    )
    row_owned = scatter_gx(row_partial.reshape(16, 2, columns, channels))
    row_mixed = gather_gx(complex_mix(row_owned, row_weight))
    total = arrived.sum(axis=0)
    column_owned = total[: 2 * half].reshape(2, half, channels)
    coarse_own = total[2 * half :].reshape(coarse_columns, coarse_rows, channels).transpose(1, 0, 2)
    column_mixed = exchange_gy(
        copies(complex_mix(column_owned, column_weight).reshape(2 * half, channels), 16)
    )
    row_field = jnp.dot(
        row_basis.T, row_mixed.reshape(32, columns * channels), precision=highest
    ) * (1.0 / math.sqrt(MODES_X))
    column_field = jnp.einsum(
        "ry,rxc->xyc", column_basis, from_gy(column_mixed), precision=highest
    ) * (1.0 / math.sqrt(MODES_Y))
    summed = (
        row_field.reshape(rows, columns, channels)
        + column_field
        + upsample(coarse_own, rows, columns, channels)
    )
    ffn_input = summed.reshape(cells_flat, channels).astype(jnp.bfloat16)
    hidden_before = jnp.einsum(
        "nc,fc->nf", ffn_input, lift_turned, preferred_element_type=jnp.float32
    )
    hidden_after = gelu_value(hidden_before).astype(jnp.bfloat16)
    cotangent_rows = cotangent.reshape(cells_flat, channels)
    drop_partial = jnp.einsum(
        "nf,nc->fc", hidden_after, cotangent_rows, preferred_element_type=jnp.float32
    )
    after_grad = jnp.einsum(
        "nc,fc->nf", cotangent_rows, drop_turned, preferred_element_type=jnp.float32
    )
    before_grad = (after_grad * gelu_slope(hidden_before)).astype(jnp.bfloat16)
    lift_partial = jnp.einsum(
        "nf,nc->fc", before_grad, ffn_input, preferred_element_type=jnp.float32
    )
    summed_grad = jnp.einsum(
        "nf,fc->nc", before_grad, lift_turned, preferred_element_type=jnp.float32
    )
    summed_cells = summed_grad.reshape(rows, columns, channels)
    row_back_partial = jnp.dot(
        row_basis, summed_grad.reshape(rows, columns * channels), precision=highest
    ) * (1.0 / math.sqrt(MODES_X))
    column_back_partial = jnp.einsum(
        "ry,xyc->rxc", column_basis, summed_cells, precision=highest
    ) * (1.0 / math.sqrt(MODES_Y))
    coarse_grad_own = summed_cells.reshape(coarse_rows, POOL, coarse_columns, POOL, channels).sum(
        axis=(1, 3)
    )
    gy_arrived = exchange_gy(
        jnp.concatenate(
            [
                to_gy(column_back_partial.reshape(MODES_Y, 2, rows, channels)),
                copies(coarse_grad_own.reshape(coarse_rows * coarse_columns, channels), 16),
            ],
            axis=1,
        )
    )
    gx_arrived = scatter_gx(
        jnp.concatenate(
            [
                row_back_partial.reshape(16, 2 * columns, channels),
                lift_partial.reshape(16, units, channels),
                drop_partial.reshape(16, units, channels),
            ],
            axis=1,
        )
    )
    row_back = gx_arrived[: 2 * columns].reshape(2, columns, channels)
    net_share = gx_arrived[2 * columns :]
    row_weight_partial, row_spec_grad = complex_back(row_owned, row_back, row_weight)
    column_back = gy_arrived[:, : 2 * half].sum(axis=0).reshape(2, half, channels)
    column_weight_partial, column_spec_grad = complex_back(column_owned, column_back, column_weight)
    coarse_grad = gy_arrived[:, 2 * half :].reshape(16, coarse_rows, coarse_columns, channels)
    coarse_grad = coarse_grad.transpose(1, 0, 2, 3).reshape(
        coarse_rows, 16 * coarse_columns, channels
    )
    coarse_act_grad = jnp.einsum("jk,ijc->ikc", own_mixing, coarse_grad, precision=highest)
    mixing_partial = jnp.einsum("ijc,ikc->kj", coarse_grad, coarse_act, precision=highest)
    coarse_pre_grad = coarse_act_grad * gelu_slope(coarse_pre)
    coarse_weight_partial = jnp.einsum("ijc,ijd->cd", pooled, coarse_pre_grad, precision=highest)
    pooled_grad = jnp.einsum("ijd,cd->ijc", coarse_pre_grad, coarse_float, precision=highest) * (
        1.0 / POOL
    )
    column_rows = 2 * half
    gy_back = exchange_gy(
        jnp.concatenate(
            [
                copies(column_spec_grad.reshape(column_rows, channels), 16),
                row_weight_partial.reshape(16, 16, channels),
                net_share.reshape(16, 4, channels),
                copies(mixing_partial.reshape(2, channels), 16),
                jnp.zeros((16, 2, channels), jnp.float32),
            ],
            axis=1,
        )
    )
    weights_out = jnp.take(
        jnp.concatenate(
            [
                column_weight_partial.reshape(16, 16, channels),
                coarse_weight_partial.reshape(16, 8, channels),
            ],
            axis=1,
        ),
        order,
        axis=0,
    )
    spec = row_spec_grad.reshape(2 * columns, channels)
    sums = weights_out.reshape(4, 4, 24, channels)
    specs = [spec]
    kept = sums[:, 0]
    for k in (3, 2, 1):
        block = lax.ppermute(
            jnp.concatenate([spec, sums[:, k].reshape(4 * 24, channels)]), "x", x_step(k)
        )
        specs.append(block[: 2 * columns])
        kept = kept + block[2 * columns :].reshape(4, 24, channels)
    specs = jnp.concatenate(specs)
    kept = kept.reshape(2, 2, 24, channels)
    length = specs.shape[0]
    block = lax.ppermute(
        jnp.concatenate([specs, kept[:, 1].reshape(48, channels)]), "yl", SWAP
    )
    specs = jnp.concatenate([specs, block[:length]])
    kept = kept[:, 0] + block[length:].reshape(2, 24, channels)
    length = specs.shape[0]
    block = lax.ppermute(jnp.concatenate([specs, kept[1]]), "co", SWAP)
    row_spec_full = jnp.concatenate([specs, block[:length]])
    weights_own = kept[0] + block[length:]
    column_spec_full = gy_back[:, :column_rows]
    row_weight_own = gy_back[:, column_rows : column_rows + 16].sum(axis=0)
    net_own = gy_back[:, column_rows + 16 : column_rows + 20].sum(axis=0)
    mixing_rows = gy_back[:, column_rows + 20 : column_rows + 22].reshape(32, channels)
    last = exchange_gy(
        copies(
            jnp.concatenate(
                [row_weight_own, weights_own, net_own, jnp.zeros((4, channels), jnp.float32)]
            ),
            16,
        )
    )
    xmode_grad = last[:, :16].reshape(2, 1, channels, channels)
    column_weight_rows = last[:, 16:32].reshape(8, 2, 16, channels).sum(axis=1)
    coarse_weight_rows = last[:, 32:40].sum(axis=0)
    net_rows = last[:, 40:44].reshape(2 * units, channels)
    packed = jnp.concatenate(
        [
            column_weight_rows.reshape(128, channels),
            net_rows,
            coarse_weight_rows,
            mixing_rows,
        ]
    )
    chips = lax.all_to_all(copies(packed, 8), ("x", "yl"), 0, 0, tiled=True)
    other = lax.ppermute(chips, "co", SWAP)
    north = lax.axis_index("co") == 0
    full = jnp.stack(
        [jnp.where(north, chips, other), jnp.where(north, other, chips)], axis=1
    ).reshape(16, packed.shape[0], channels)
    ymode_grad = (
        full[:, :128]
        .reshape(2, 8, 8, 16, channels)
        .transpose(0, 2, 1, 3, 4)
        .reshape(2, MODES_Y, channels, channels)
    )
    lift_grad = full[:, 128 : 128 + units].reshape(16 * units, channels).T
    drop_grad = full[:, 128 + units : 128 + 2 * units].reshape(16 * units, channels)
    coarse_weight_grad = full[:, 192:200].reshape(channels, channels)
    coarse_mix_grad = full[:, 200:232].sum(axis=0).reshape(64, 64).T
    row_cell_grad = jnp.dot(
        row_basis.T, row_spec_full.reshape(32, columns * channels), precision=highest
    ) * (1.0 / math.sqrt(row_total))
    column_cell_grad = jnp.einsum(
        "ry,rxc->xyc", column_basis, from_gy(column_spec_full), precision=highest
    ) * (1.0 / math.sqrt(column_total))
    cell_grad = (
        cotangent.astype(jnp.float32)
        + row_cell_grad.reshape(rows, columns, channels)
        + column_cell_grad
        + upsample(pooled_grad, rows, columns, channels)
    ).astype(jnp.bfloat16)
    return (
        cell_grad,
        lift_grad,
        drop_grad,
        xmode_grad,
        ymode_grad,
        coarse_weight_grad,
        coarse_mix_grad,
    )


def solution(mesh):
    split = Mesh(mesh.devices.reshape(4, 2, 2, 2, 8), ("x", "yl", "co", "yh", "z"))
    placed = (
        P(GX, GY, None),
        P(GX, GY, None),
        P(),
        P(),
        P(None, GX, None, None),
        P(),
        P(),
        P(),
    )
    return jax.shard_map(
        on_device,
        mesh=split,
        in_specs=placed,
        out_specs=(P(GX, GY, None), P(), P(), P(None, GX, None, None), P(), P(), P()),
        check_vma=False,
    )
```

```python
import functools
import math

import jax
import jax.numpy as jnp
from jax import lax
from jax.experimental import pallas as pl
from jax.experimental.pallas import tpu as pltpu
from jax.sharding import Mesh
from jax.sharding import PartitionSpec as P

MODES_X = 16
MODES_Y = 8
POOL = 16
GX = ("x", "yl", "co")
GY = ("yh", "z")

gelu_scale = 0.7978845608028654
gelu_cubic = 0.044715
highest = lax.Precision.HIGHEST


f32 = jnp.float32
bf16 = jnp.bfloat16
STEPS = 16
SPAN = 8
NT = (((1,), (1,)), ((), ()))
NN = (((1,), (0,)), ((), ()))


def split(values):
    high = values.astype(bf16)
    return high, (values - high.astype(f32)).astype(bf16)


def dot(a, b, dims=NN):
    return lax.dot_general(a, b, dims, preferred_element_type=f32)


def tables_kernel(rb_ref, cb_ref, rt_ref, ct_ref, rbk_ref, cbk_ref):
    def ids(shape, dim):
        return lax.broadcasted_iota(jnp.int32, shape, dim)

    def hot(shape, a, b):
        return jnp.where(a(ids(shape, 0)) == b(ids(shape, 1)), 1.0, 0.0).astype(bf16)

    row_spread = hot((1024, 128), lambda n: n // 8, lambda x: x)
    row_modes = hot((256, 32), lambda k: k // 8, lambda r: r)
    column_spread = hot((512, 64), lambda n: n % 64, lambda y: y)
    column_modes = hot((128, 16), lambda k: k // 8, lambda r: r)
    row_mask = ids((1024, 256), 0) % 8 == ids((1024, 256), 1) % 8
    row_mask_t = ids((256, 1024), 0) % 8 == ids((256, 1024), 1) % 8
    column_mask = ids((512, 128), 0) // 64 == ids((512, 128), 1) % 8
    column_mask_t = ids((128, 512), 0) % 8 == ids((128, 512), 1) // 64
    row_high, row_low = split(rb_ref[...])
    column_high, column_low = split(cb_ref[...])
    for at, kind in enumerate((0, 0, 1)):
        r = (row_high, row_low)[kind]
        c = (column_high, column_low)[kind]
        wide = dot(row_modes, r).astype(bf16)
        rt_ref[:, at * 256 : at * 256 + 256] = jnp.where(row_mask, dot(row_spread, wide, NT), 0.0).astype(bf16)
        rbk_ref[:, at * 1024 : at * 1024 + 1024] = jnp.where(row_mask_t, dot(wide, row_spread, NT), 0.0).astype(bf16)
        tall = dot(column_modes, c).astype(bf16)
        ct_ref[:, at * 128 : at * 128 + 128] = jnp.where(column_mask, dot(column_spread, tall, NT), 0.0).astype(bf16)
        cbk_ref[:, at * 512 : at * 512 + 512] = jnp.where(column_mask_t, dot(tall, column_spread, NT), 0.0).astype(bf16)


def spread_tables(row_basis, column_basis):
    return pl.pallas_call(
        tables_kernel,
        out_shape=[
            jax.ShapeDtypeStruct((1024, 256 * 3), bf16),
            jax.ShapeDtypeStruct((512, 128 * 3), bf16),
            jax.ShapeDtypeStruct((256, 1024 * 3), bf16),
            jax.ShapeDtypeStruct((128, 512 * 3), bf16),
        ],
        compiler_params=pltpu.CompilerParams(vmem_limit_bytes=48 * 1024 * 1024),
        name="tables",
    )(row_basis, column_basis)


def stacked(values):
    high, low = split(values)
    return jnp.concatenate([high, low, high], axis=0)


def row_fields(row_ref, table_ref, field):
    for b in range(8):
        block = row_ref[:, b * 8 : b * 8 + 8, :].reshape(256, 128)
        field[:, b * 8 : b * 8 + 8, :] = dot(table_ref[...], stacked(block)).reshape(128, 8, 128)


def column_block(column_ref, step):
    group = step // 8
    start = (step % 8) * 8
    pieces = []
    for m in range(8):
        for p in range(2):
            at = pl.multiple_of(p * 64 + start, 8)
            pieces.append(column_ref[2 * m + group, pl.ds(at, 8), :])
    return jnp.concatenate(pieces, axis=0)


def coarse_rows(coarse_ref, step):
    block = coarse_ref[step // 2]
    return jnp.concatenate(
        [jnp.broadcast_to(block[j : j + 1], (16, 128)) for j in range(4)], axis=0
    )


def net_kernel(
    row_ref, column_ref, coarse_ref, cot_ref, lift_ref, drop_ref, liftT_ref,
    rt_ref, ct_ref, rb_ref, cb_ref,
    x_ref, y_ref, field, lift_sum, drop_sum, coarse_sum, *, chunk,
):
    step = pl.program_id(0)

    @pl.when(step == 0)
    def _():
        row_fields(row_ref, rt_ref, field)
        lift_sum[...] = jnp.zeros_like(lift_sum)
        drop_sum[...] = jnp.zeros_like(drop_sum)
        coarse_sum[...] = jnp.zeros_like(coarse_sum)

    x0 = pl.multiple_of(step * 8, 8)
    summed = field[pl.ds(x0, 8)] + dot(ct_ref[...], stacked(column_block(column_ref, step))).reshape(
        8, 64, 128
    )
    summed = summed + coarse_rows(coarse_ref, step)[None]
    cells_in = summed.reshape(512, 128).astype(bf16)
    cot = cot_ref[...].reshape(512, 128)
    grad = jnp.zeros((128, 512), f32)
    for k in range(512 // chunk):
        at = slice(k * chunk, (k + 1) * chunk)
        before = dot(lift_ref[at, :], cells_in, NT)
        after_grad = dot(drop_ref[at, :], cot, NT)
        square = before * before
        tangent = jnp.tanh(before * (gelu_scale + (gelu_scale * gelu_cubic) * square))
        gate = 0.5 + 0.5 * tangent
        after = before * gate
        bend = 2.0 * gelu_scale + (6.0 * gelu_scale * gelu_cubic) * square
        slope = gate + after * (1.0 - gate) * bend
        after = after.astype(bf16)
        before_grad = (after_grad * slope).astype(bf16)
        drop_sum[at, :] += dot(after, cot)
        lift_sum[at, :] += dot(before_grad, cells_in)
        grad = grad + dot(liftT_ref[:, at], before_grad)
    grad = grad.T
    cube = grad.reshape(8, 64, 128)
    field[pl.ds(x0, 8)] = cube
    back = dot(cb_ref[...], stacked(grad))
    group = step // 8
    start = (step % 8) * 8
    for m in range(8):
        for p in range(2):
            at = pl.multiple_of(p * 64 + start, 8)
            i = (m * 2 + p) * 8
            y_ref[2 * m + group, pl.ds(at, 8), :] = back[i : i + 8]
    across = cube.sum(axis=0)
    sums = [across[j * 16 : j * 16 + 16].sum(axis=0, keepdims=True) for j in range(4)]
    coarse_sum[step // 2, 0:4, :] += jnp.concatenate(sums, axis=0)

    @pl.when(step == STEPS - 1)
    def _():
        for b in range(8):
            block = field[:, b * 8 : b * 8 + 8, :].reshape(1024, 128)
            out = dot(rb_ref[...], stacked(block))
            for j in range(16):
                for p in range(2):
                    i = (j * 2 + p) * 8
                    x_ref[j, p * 64 + b * 8 : p * 64 + b * 8 + 8, :] = out[i : i + 8]
        for j in range(16):
            x_ref[j, 128:160, :] = lift_sum[j * 32 : j * 32 + 32, :]
            x_ref[j, 160:192, :] = drop_sum[j * 32 : j * 32 + 32, :]
        coarse = jnp.concatenate([coarse_sum[i, 0:4, :] for i in range(8)], axis=0)
        for d in range(16):
            y_ref[d, 128:160, :] = coarse


def net(row_mixed, column_mixed, coarse_own, cotangent, lift, drop, tables, chunk=512):
    rt, ct, rb, cb = tables
    whole = pl.BlockSpec(memory_space=pltpu.VMEM)
    return pl.pallas_call(
        functools.partial(net_kernel, chunk=chunk),
        grid=(STEPS,),
        in_specs=[whole] * 3
        + [pl.BlockSpec((8, 64, 128), lambda i: (i, 0, 0))]
        + [whole] * 7,
        out_specs=[whole, whole],
        out_shape=[
            jax.ShapeDtypeStruct((16, 192, 128), f32),
            jax.ShapeDtypeStruct((16, 160, 128), f32),
        ],
        scratch_shapes=[
            pltpu.VMEM((128, 64, 128), f32),
            pltpu.VMEM((512, 128), f32),
            pltpu.VMEM((512, 128), f32),
            pltpu.VMEM((8, 8, 128), f32),
        ],
        compiler_params=pltpu.CompilerParams(
            dimension_semantics=("arbitrary",), vmem_limit_bytes=48 * 1024 * 1024
        ),
        name="net",
    )(row_mixed, column_mixed, coarse_own, cotangent, lift, drop, lift.T, rt, ct, rb, cb)


def input_kernel(row_ref, column_ref, coarse_ref, cot_ref, rt_ref, ct_ref, out_ref, field):
    step = pl.program_id(0)

    @pl.when(step == 0)
    def _():
        row_fields(row_ref, rt_ref, field)

    x0 = pl.multiple_of(step * 8, 8)
    total = field[pl.ds(x0, 8)] + dot(ct_ref[...], stacked(column_block(column_ref, step))).reshape(
        8, 64, 128
    )
    total = total + coarse_rows(coarse_ref, step)[None] + cot_ref[...].astype(f32)
    out_ref[...] = total.astype(bf16)


def input_grad(row_spec, column_spec, coarse, cotangent, tables):
    rt, ct = tables
    whole = pl.BlockSpec(memory_space=pltpu.VMEM)
    block = pl.BlockSpec((8, 64, 128), lambda i: (i, 0, 0))
    return pl.pallas_call(
        input_kernel,
        grid=(STEPS,),
        in_specs=[whole] * 3 + [block] + [whole] * 2,
        out_specs=block,
        out_shape=jax.ShapeDtypeStruct((128, 64, 128), bf16),
        scratch_shapes=[pltpu.VMEM((128, 64, 128), f32)],
        compiler_params=pltpu.CompilerParams(
            dimension_semantics=("arbitrary",), vmem_limit_bytes=48 * 1024 * 1024
        ),
        name="input_grad",
    )(row_spec, column_spec, coarse, cotangent, rt, ct)


def gelu_value(values):
    tangent = jnp.tanh(gelu_scale * (values + gelu_cubic * values * values * values))
    return 0.5 * values * (1.0 + tangent)


def gelu_slope(values):
    tangent = jnp.tanh(gelu_scale * (values + gelu_cubic * values * values * values))
    return 0.5 * (1.0 + tangent) + 0.5 * values * (1.0 - tangent * tangent) * gelu_scale * (
        1.0 + 3.0 * gelu_cubic * values * values
    )


def basis_of(frequency, length, offset, extent):
    places = offset + jnp.arange(extent, dtype=jnp.int32)
    phase_index = frequency[:, None] * places[None, :] % length
    angles = phase_index.astype(jnp.float32) * (2.0 * math.pi / length)
    return jnp.stack([jnp.cos(angles), -jnp.sin(angles)], axis=1)


def x_step(step):
    return [(i, (i + step) % 4) for i in range(4)]


SWAP = [(0, 1), (1, 0)]


def relative_modes():
    j = jnp.arange(16, dtype=jnp.int32)
    x = (lax.axis_index("x") + j % 4) % 4
    yl = (lax.axis_index("yl") + j // 4) % 2
    co = (lax.axis_index("co") + j // 8) % 2
    return x * 4 + yl * 2 + co


def scatter_gx(parts):
    s = parts[:8] + lax.ppermute(parts[8:], "co", SWAP)
    s = s[:4] + lax.ppermute(s[4:], "yl", SWAP)
    arrived = [lax.ppermute(s[k], "x", x_step(k)) for k in (1, 2, 3)]
    return s[0] + arrived[0] + arrived[1] + arrived[2]


def gather_gx(own):
    g = jnp.stack([own] + [lax.ppermute(own, "x", x_step(-k)) for k in (1, 2, 3)])
    g = jnp.concatenate([g, lax.ppermute(g, "yl", SWAP)])
    return jnp.concatenate([g, lax.ppermute(g, "co", SWAP)])


def exchange_gy(parts):
    return lax.all_to_all(parts, GY, 0, 0, tiled=True)


def copies(block, count):
    return jnp.broadcast_to(block[None], (count, *block.shape))


def complex_mix(spectrum, weights):
    def product(former, latter):
        return jnp.einsum("rc,cd->rd", former, latter, precision=highest)

    return jnp.stack(
        [
            product(spectrum[0], weights[0]) - product(spectrum[1], weights[1]),
            product(spectrum[0], weights[1]) + product(spectrum[1], weights[0]),
        ]
    )


def complex_back(spectrum, gradient, weights):
    def over_cells(former, latter):
        return jnp.einsum("rc,rd->cd", former, latter, precision=highest)

    def over_channels(former, latter):
        return jnp.einsum("rd,cd->rc", former, latter, precision=highest)

    weight = jnp.stack(
        [
            over_cells(spectrum[0], gradient[0]) + over_cells(spectrum[1], gradient[1]),
            over_cells(spectrum[0], gradient[1]) - over_cells(spectrum[1], gradient[0]),
        ]
    )
    spec = jnp.stack(
        [
            over_channels(gradient[0], weights[0]) + over_channels(gradient[1], weights[1]),
            over_channels(gradient[1], weights[0]) - over_channels(gradient[0], weights[1]),
        ]
    )
    return weight, spec


def on_device(
    cells,
    cotangent,
    lift_weight,
    drop_weight,
    xmode_weight,
    ymode_weight,
    coarse_weight,
    coarse_mix,
):
    rows, columns, channels = cells.shape
    row_total = rows * 16
    column_total = columns * 16
    coarse_rows = rows // POOL
    coarse_columns = columns // POOL
    half = rows // 2
    gx = lax.axis_index(GX)
    gy = lax.axis_index(GY)
    order = relative_modes()
    row_basis = basis_of(order, row_total, gx * rows, rows).reshape(32, rows)
    column_basis = basis_of(
        jnp.arange(MODES_Y, dtype=jnp.int32), column_total, gy * columns, columns
    ).reshape(16, columns)
    row_weight = xmode_weight[:, 0].astype(jnp.float32)
    column_weight = lax.dynamic_index_in_dim(ymode_weight, gy // 2, 1, keepdims=False).astype(
        jnp.float32
    )
    coarse_float = coarse_weight.astype(jnp.float32)
    mixing = coarse_mix.astype(jnp.float32)
    own_mixing = lax.dynamic_slice_in_dim(mixing, gy * coarse_columns, coarse_columns, 1)
    units = lift_weight.shape[1] // 16
    lift_turned = jnp.take(lift_weight.T.reshape(16, units, channels), order, axis=0).reshape(
        16 * units, channels
    )
    drop_turned = jnp.take(drop_weight.reshape(16, units, channels), order, axis=0).reshape(
        16 * units, channels
    )

    def to_gy(by_part):
        return (
            by_part.reshape(MODES_Y, 2, 2, half, channels)
            .transpose(0, 2, 1, 3, 4)
            .reshape(16, 2 * half, channels)
        )

    row_partial = jnp.dot(
        row_basis.astype(jnp.bfloat16),
        cells.reshape(rows, columns * channels),
        preferred_element_type=jnp.float32,
    ) * (1.0 / math.sqrt(row_total))
    column_partial = jnp.einsum(
        "ry,xyc->rxc", column_basis.astype(jnp.bfloat16), cells, preferred_element_type=jnp.float32
    ) * (1.0 / math.sqrt(column_total))
    pooled = cells.astype(jnp.float32).reshape(
        coarse_rows, POOL, coarse_columns, POOL, channels
    ).sum(axis=(1, 3)) * (1.0 / POOL)
    coarse_pre = jnp.einsum("ijc,cd->ijd", pooled, coarse_float, precision=highest)
    coarse_act = gelu_value(coarse_pre)
    coarse_share = jnp.einsum("jk,ikc->jic", own_mixing, coarse_act, precision=highest)
    coarse_share = coarse_share.reshape(16, coarse_columns * coarse_rows, channels)
    arrived = exchange_gy(
        jnp.concatenate(
            [to_gy(column_partial.reshape(MODES_Y, 2, rows, channels)), coarse_share], axis=1
        )
    )
    row_owned = scatter_gx(row_partial.reshape(16, 2, columns, channels))
    row_mixed = gather_gx(complex_mix(row_owned, row_weight))
    total = arrived.sum(axis=0)
    column_owned = total[: 2 * half].reshape(2, half, channels)
    coarse_own = total[2 * half :].reshape(coarse_columns, coarse_rows, channels).transpose(1, 0, 2)
    column_mixed = exchange_gy(
        copies(complex_mix(column_owned, column_weight).reshape(2 * half, channels), 16)
    )
    tables = spread_tables(
        row_basis * (1.0 / math.sqrt(MODES_X)), column_basis * (1.0 / math.sqrt(MODES_Y))
    )
    to_rows, to_columns = net(
        row_mixed.reshape(32, columns, channels),
        column_mixed,
        coarse_own,
        cotangent,
        lift_turned,
        drop_turned,
        tables,
    )
    gy_arrived = exchange_gy(to_columns)
    gx_arrived = scatter_gx(to_rows)
    row_back = gx_arrived[: 2 * columns].reshape(2, columns, channels)
    net_share = gx_arrived[2 * columns :]
    row_weight_partial, row_spec_grad = complex_back(row_owned, row_back, row_weight)
    row_spec_grad = row_spec_grad * math.sqrt(MODES_X / row_total)
    column_back = gy_arrived[:, : 2 * half].sum(axis=0).reshape(2, half, channels)
    column_weight_partial, column_spec_grad = complex_back(column_owned, column_back, column_weight)
    column_spec_grad = column_spec_grad * math.sqrt(MODES_Y / column_total)
    coarse_grad = gy_arrived[:, 2 * half :].reshape(16, coarse_rows, coarse_columns, channels)
    coarse_grad = coarse_grad.transpose(1, 0, 2, 3).reshape(
        coarse_rows, 16 * coarse_columns, channels
    )
    coarse_act_grad = jnp.einsum("jk,ijc->ikc", own_mixing, coarse_grad, precision=highest)
    mixing_partial = jnp.einsum("ijc,ikc->kj", coarse_grad, coarse_act, precision=highest)
    coarse_pre_grad = coarse_act_grad * gelu_slope(coarse_pre)
    coarse_weight_partial = jnp.einsum("ijc,ijd->cd", pooled, coarse_pre_grad, precision=highest)
    pooled_grad = jnp.einsum("ijd,cd->ijc", coarse_pre_grad, coarse_float, precision=highest) * (
        1.0 / POOL
    )
    column_rows = 2 * half
    gy_back = exchange_gy(
        jnp.concatenate(
            [
                copies(column_spec_grad.reshape(column_rows, channels), 16),
                row_weight_partial.reshape(16, 16, channels),
                net_share.reshape(16, 4, channels),
                copies(mixing_partial.reshape(2, channels), 16),
                jnp.zeros((16, 2, channels), jnp.float32),
            ],
            axis=1,
        )
    )
    weights_out = jnp.take(
        jnp.concatenate(
            [
                column_weight_partial.reshape(16, 16, channels),
                coarse_weight_partial.reshape(16, 8, channels),
            ],
            axis=1,
        ),
        order,
        axis=0,
    )
    spec = row_spec_grad.reshape(2 * columns, channels)
    sums = weights_out.reshape(4, 4, 24, channels)
    specs = [spec]
    kept = sums[:, 0]
    for k in (3, 2, 1):
        block = lax.ppermute(
            jnp.concatenate([spec, sums[:, k].reshape(4 * 24, channels)]), "x", x_step(k)
        )
        specs.append(block[: 2 * columns])
        kept = kept + block[2 * columns :].reshape(4, 24, channels)
    specs = jnp.concatenate(specs)
    kept = kept.reshape(2, 2, 24, channels)
    length = specs.shape[0]
    block = lax.ppermute(
        jnp.concatenate([specs, kept[:, 1].reshape(48, channels)]), "yl", SWAP
    )
    specs = jnp.concatenate([specs, block[:length]])
    kept = kept[:, 0] + block[length:].reshape(2, 24, channels)
    length = specs.shape[0]
    block = lax.ppermute(jnp.concatenate([specs, kept[1]]), "co", SWAP)
    row_spec_full = jnp.concatenate([specs, block[:length]])
    weights_own = kept[0] + block[length:]
    row_weight_own = gy_back[:, column_rows : column_rows + 16].sum(axis=0)
    net_own = gy_back[:, column_rows + 16 : column_rows + 20].sum(axis=0)
    mixing_rows = gy_back[:, column_rows + 20 : column_rows + 22].reshape(32, channels)
    last = exchange_gy(
        copies(
            jnp.concatenate(
                [row_weight_own, weights_own, net_own, jnp.zeros((4, channels), jnp.float32)]
            ),
            16,
        )
    )
    xmode_grad = last[:, :16].reshape(2, 1, channels, channels)
    column_weight_rows = last[:, 16:32].reshape(8, 2, 16, channels).sum(axis=1)
    coarse_weight_rows = last[:, 32:40].sum(axis=0)
    net_rows = last[:, 40:44].reshape(2 * units, channels)
    packed = jnp.concatenate(
        [
            column_weight_rows.reshape(128, channels),
            net_rows,
            coarse_weight_rows,
            mixing_rows,
        ]
    )
    chips = lax.all_to_all(copies(packed, 8), ("x", "yl"), 0, 0, tiled=True)
    other = lax.ppermute(chips, "co", SWAP)
    north = lax.axis_index("co") == 0
    full = jnp.stack(
        [jnp.where(north, chips, other), jnp.where(north, other, chips)], axis=1
    ).reshape(16, packed.shape[0], channels)
    ymode_grad = (
        full[:, :128]
        .reshape(2, 8, 8, 16, channels)
        .transpose(0, 2, 1, 3, 4)
        .reshape(2, MODES_Y, channels, channels)
    )
    lift_grad = full[:, 128 : 128 + units].reshape(16 * units, channels).T
    drop_grad = full[:, 128 + units : 128 + 2 * units].reshape(16 * units, channels)
    coarse_weight_grad = full[:, 192:200].reshape(channels, channels)
    coarse_mix_grad = full[:, 200:232].sum(axis=0).reshape(64, 64).T
    cell_grad = input_grad(
        row_spec_full.reshape(32, columns, channels),
        gy_back,
        pooled_grad,
        cotangent,
        tables[:2],
    )
    return (
        cell_grad,
        lift_grad,
        drop_grad,
        xmode_grad,
        ymode_grad,
        coarse_weight_grad,
        coarse_mix_grad,
    )


def solution(mesh):
    split = Mesh(mesh.devices.reshape(4, 2, 2, 2, 8), ("x", "yl", "co", "yh", "z"))
    placed = (
        P(GX, GY, None),
        P(GX, GY, None),
        P(),
        P(),
        P(None, GX, None, None),
        P(),
        P(),
        P(),
    )
    return jax.shard_map(
        on_device,
        mesh=split,
        in_specs=placed,
        out_specs=(P(GX, GY, None), P(), P(), P(None, GX, None, None), P(), P(), P()),
        check_vma=False,
    )
```
